32 devices in a mesh: tok: 16 (over z, y, x), blk: 2 (over core).
Axes of the slice: x: 2, y: 2, z: 4, core: 2. Of those that a mesh axis runs over, the one named last changes fastest.
Arguments:
- activations: bfloat16 [4096, 2048], P('tok', 'blk'), may hold values from -16 to 16
Outputs:
- factored: float32 [2048, 2048], P('blk', 'tok')
The draws below stay inside these ranges and needn't reach their ends.
All inputs are finite; a program needn't handle non-finite values.
Results may differ from the reference program's by a relative error of at most 0.0003.
Values may be sent and summed in bfloat16 or wider, within the bound.
A program may use at most 64 MiB of HBM per device.

```python
import math
import jax
import jax.numpy as jnp
from jax import lax

D = 2048
STEPS = 4
TOKENS = 4096
N_TOK = 16


def draw_activations(key, part):
    first, second, third, fourth = jax.random.split(key, 4)
    scales = jnp.exp(jax.random.uniform(first, (D,), jnp.float32, math.log(0.3), math.log(3.0)))
    base = jax.random.normal(second, (TOKENS, D), jnp.float32)
    shared_weight = 0.6
    common = jax.random.normal(third, (TOKENS, 16), jnp.float32)
    mixing = jax.random.normal(fourth, (16, D), jnp.float32) * 0.25
    values = (base + shared_weight * jnp.dot(common, mixing)) * scales
    return jnp.clip(values, -16.0, 16.0).astype(jnp.bfloat16)


def setup_inputs(seed: int = 0) -> dict:
    key_of = jax.random.split(jax.random.key(seed), 2)
    return {
        "activations": draw_activations(jax.random.fold_in(key_of[1], 71), 0),
    }


def reference(activations):
    total = activations.shape[0]
    hessian = lax.dot_general(activations.astype(jnp.float32), activations.astype(jnp.float32), (((0,), (0,)), ((), ())), preferred_element_type=jnp.float32) * (2.0 / total)
    damping = 0.01 * jnp.mean(jnp.diagonal(hessian))
    damped = hessian + damping * jnp.eye(D, dtype=jnp.float32)
    cols = STEPS * (D // N_TOK)
    leading = jnp.linalg.cholesky(damped[:cols, :cols])
    lower = jax.scipy.linalg.solve_triangular(leading, damped[cols:, :cols].T, lower=True).T
    schur = damped[cols:, cols:] - jnp.dot(lower, lower.T, precision=lax.Precision.HIGHEST)
    left_part = jnp.concatenate([leading, lower], 0)
    right_part = jnp.concatenate([jnp.zeros((cols, D - cols), jnp.float32), jnp.tril(schur)], 0)
    return jnp.concatenate([left_part, right_part], 1)
```

```python
import functools
import jax
import jax.numpy as jnp
from jax import lax
from jax.experimental import pallas as pl
from jax.experimental.pallas import tpu as pltpu
from jax.sharding import PartitionSpec as P

STEPS = 4
GROUP = 8
HIGH = lax.Precision.HIGHEST


def factor_block(block):
    size = block.shape[0]
    count = size // GROUP
    shape = (GROUP, size)
    lanes = lax.broadcasted_iota(jnp.int32, shape, 1)
    subs = lax.broadcasted_iota(jnp.int32, shape, 0)
    left = [block[GROUP * g : GROUP * (g + 1), :] for g in range(count)]
    right = [jnp.where(lanes == subs + GROUP * g, 1.0, 0.0) for g in range(count)]

    def column(rows, j):
        return jnp.broadcast_to(rows[:, j : j + 1], shape)

    def row(rows, i):
        return jnp.broadcast_to(rows[i : i + 1, :], shape)

    for g in range(count):
        base = GROUP * g
        cols = [column(left[g], base + j) for j in range(GROUP)]
        a = [[row(cols[j], i) for j in range(i + 1)] for i in range(GROUP)]
        low = [[None] * GROUP for _ in range(GROUP)]
        inv = [None] * GROUP
        for j in range(GROUP):
            inv[j] = lax.rsqrt(a[j][j])
            for i in range(j + 1, GROUP):
                low[i][j] = a[i][j] * inv[j]
            for i in range(j + 1, GROUP):
                for m in range(j + 1, i + 1):
                    a[i][m] = a[i][m] - low[i][j] * low[m][j]
        r_left = [row(left[g], i) for i in range(GROUP)]
        r_right = [row(right[g], i) for i in range(GROUP)]
        u_left, u_right = [], []
        for i in range(GROUP):
            for rows, done in ((r_left, u_left), (r_right, u_right)):
                total = rows[i]
                for m in range(i):
                    total = total - low[i][m] * done[m]
                done.append(total * inv[i])
        g_left, g_right = [None] * GROUP, [None] * GROUP
        for i in reversed(range(GROUP)):
            for rows, done in ((u_left, g_left), (u_right, g_right)):
                total = rows[i]
                for m in range(i + 1, GROUP):
                    total = total - low[m][i] * done[m]
                done[i] = total * inv[i]
        out_left, out_right = u_left[0], u_right[0]
        for i in range(1, GROUP):
            out_left = jnp.where(subs == i, u_left[i], out_left)
            out_right = jnp.where(subs == i, u_right[i], out_right)
        for h in range(g + 1, count):
            rows = [column(left[h], base + j) for j in range(GROUP)]
            for j in range(GROUP):
                left[h] = left[h] - rows[j] * g_left[j]
                right[h] = right[h] - rows[j] * g_right[j]
        left[g], right[g] = out_left, out_right
    return jnp.concatenate(left, 0), jnp.concatenate(right, 0)


def factor_kernel(width, a_ref, u_ref, m_ref):
    n = a_ref.shape[0]
    m_ref[:, :n] = a_ref[...]
    ids = lax.broadcasted_iota(jnp.int32, (n, n), 0) == lax.broadcasted_iota(jnp.int32, (n, n), 1)
    m_ref[:, n:] = jnp.where(ids, 1.0, 0.0)

    for k in range(n // width):
        at = k * width
        _, inverse = factor_block(m_ref[at : at + width, at : at + width])
        upper = jnp.dot(inverse, m_ref[at : at + width, :], precision=HIGH, preferred_element_type=jnp.float32)
        col_ids = lax.broadcasted_iota(jnp.int32, upper.shape, 1)
        row_ids = lax.broadcasted_iota(jnp.int32, upper.shape, 0) + at
        upper = jnp.where((col_ids >= row_ids) & (col_ids <= row_ids + n), upper, 0.0)
        u_ref[at : at + width, :] = upper
        if at + width < n:
            m_ref[at + width :, :] -= lax.dot_general(
                upper[:, at + width : n], upper, (((0,), (0,)), ((), ())),
                precision=HIGH, preferred_element_type=jnp.float32,
            )


def factor(a):
    n = a.shape[0]
    width = min(128, n)
    out = pl.pallas_call(
        functools.partial(factor_kernel, width),
        out_shape=jax.ShapeDtypeStruct((n, 2 * n), jnp.float32),
        in_specs=[pl.BlockSpec(memory_space=pltpu.VMEM)],
        out_specs=pl.BlockSpec(memory_space=pltpu.VMEM),
        scratch_shapes=[pltpu.VMEM((n, 2 * n), jnp.float32)],
        compiler_params=pltpu.CompilerParams(vmem_limit_bytes=48 * 1024 * 1024),
    )(a)
    return out[:, :n], out[:, n:]


def gram(a, b):
    return lax.dot_general(a, b, (((0,), (0,)), ((), ())), preferred_element_type=jnp.float32)


def spread(block, holder):
    return lax.psum(jnp.where(lax.axis_index("blk") == holder, block, 0), "blk")


def gather(activations, lead, strip_width):
    rows_block = activations.shape[1]
    tok_index = lax.axis_index("tok")
    own = lax.all_gather(activations, "tok", axis=0, tiled=True)
    start = tok_index * strip_width
    strip = lax.dynamic_slice_in_dim(own, lax.rem(start, rows_block), strip_width, 1)
    if lax.axis_size("blk") > 2:
        first = spread(own[:, :lead], 0)
        strip = spread(strip, start // rows_block)
    else:
        both = lax.all_gather(jnp.concatenate([own[:, :lead], strip], 1), "blk", axis=0)
        first = both[0, :, :lead]
        strip = lax.dynamic_index_in_dim(both, start // rows_block, 0, False)[:, lead:]
    square = jnp.sum(jnp.square(own.astype(jnp.float32)))
    squares = jnp.sum(lax.all_gather(jnp.broadcast_to(square, (8, 128)), "blk", axis=0)[:, 0, 0])
    return own, first, strip, squares


def finish(own, first, strip, squares, sizes):
    rows_block, full_width, strip_width, lead, total_tokens = sizes
    tok_index = lax.axis_index("tok")
    blk_index = lax.axis_index("blk")
    scale = 2.0 / total_tokens
    damping = 0.01 * squares * scale / full_width
    corner = gram(first, first) * scale
    ids = jnp.arange(lead, dtype=jnp.int32)
    corner = corner + jnp.where(ids[:, None] == ids[None, :], damping, 0.0)
    upper, inverse = factor(corner)
    side = gram(own, first) * scale
    tile = gram(own, strip) * scale
    cross = gram(strip, first) * scale
    lower_rows = lax.dot_general(side, inverse, (((1,), (1,)), ((), ())), precision=HIGH)
    lower_cols = lax.dot_general(cross, inverse, (((1,), (1,)), ((), ())), precision=HIGH)
    row_ids = blk_index * rows_block + jnp.arange(rows_block, dtype=jnp.int32)[:, None]
    col_ids = tok_index * strip_width + jnp.arange(strip_width, dtype=jnp.int32)[None, :]
    schur = tile + jnp.where(row_ids == col_ids, damping, 0.0)
    schur = schur - lax.dot_general(lower_rows, lower_cols, (((1,), (1,)), ((), ())), precision=HIGH)
    at = jnp.minimum(tok_index * strip_width, lead - strip_width)
    leading = jnp.concatenate([upper.T, jnp.zeros((max(rows_block - lead, 0), lead), jnp.float32)], 0)
    head = jnp.where(row_ids < lead, leading, lower_rows)
    head = lax.dynamic_slice_in_dim(head, at, strip_width, 1)
    result = jnp.where(col_ids < lead, head, schur)
    return jnp.where((row_ids >= col_ids) & ((row_ids >= lead) | (col_ids < lead)), result, 0.0)


def shards(activations):
    rows_block = activations.shape[1]
    tok_count = lax.axis_size("tok")
    full_width = rows_block * lax.axis_size("blk")
    strip_width = full_width // tok_count
    lead = STEPS * strip_width
    total_tokens = activations.shape[0] * tok_count
    sizes = (rows_block, full_width, strip_width, lead, total_tokens)
    return finish(*gather(activations, lead, strip_width), sizes)


def solution(mesh):
    return jax.shard_map(
        shards,
        mesh=mesh,
        in_specs=(P("tok", "blk"),),
        out_specs=P("blk", "tok"),
        check_vma=False,
    )
```

```python
import functools
import jax
import jax.numpy as jnp
from jax import lax
from jax.experimental import pallas as pl
from jax.experimental.pallas import tpu as pltpu
from jax.sharding import PartitionSpec as P

STEPS = 4
GROUP = 8
HIGH = lax.Precision.HIGHEST


def factor_block(block):
    size = block.shape[0]
    count = size // GROUP
    shape = (GROUP, size)
    lanes = lax.broadcasted_iota(jnp.int32, shape, 1)
    subs = lax.broadcasted_iota(jnp.int32, shape, 0)
    left = [block[GROUP * g : GROUP * (g + 1), :] for g in range(count)]
    right = [jnp.where(lanes == subs + GROUP * g, 1.0, 0.0) for g in range(count)]

    def column(rows, j):
        return jnp.broadcast_to(rows[:, j : j + 1], shape)

    def row(rows, i):
        return jnp.broadcast_to(rows[i : i + 1, :], shape)

    for g in range(count):
        base = GROUP * g
        cols = [column(left[g], base + j) for j in range(GROUP)]
        a = [[row(cols[j], i) for j in range(i + 1)] for i in range(GROUP)]
        low = [[None] * GROUP for _ in range(GROUP)]
        inv = [None] * GROUP
        for j in range(GROUP):
            inv[j] = lax.rsqrt(a[j][j])
            for i in range(j + 1, GROUP):
                low[i][j] = a[i][j] * inv[j]
            for i in range(j + 1, GROUP):
                for m in range(j + 1, i + 1):
                    a[i][m] = a[i][m] - low[i][j] * low[m][j]
        r_left = [row(left[g], i) for i in range(GROUP)]
        r_right = [row(right[g], i) for i in range(GROUP)]
        u_left, u_right = [], []
        for i in range(GROUP):
            for rows, done in ((r_left, u_left), (r_right, u_right)):
                total = rows[i]
                for m in range(i):
                    total = total - low[i][m] * done[m]
                done.append(total * inv[i])
        g_left, g_right = [None] * GROUP, [None] * GROUP
        for i in reversed(range(GROUP)):
            for rows, done in ((u_left, g_left), (u_right, g_right)):
                total = rows[i]
                for m in range(i + 1, GROUP):
                    total = total - low[m][i] * done[m]
                done[i] = total * inv[i]
        out_left, out_right = u_left[0], u_right[0]
        for i in range(1, GROUP):
            out_left = jnp.where(subs == i, u_left[i], out_left)
            out_right = jnp.where(subs == i, u_right[i], out_right)
        for h in range(g + 1, count):
            rows = [column(left[h], base + j) for j in range(GROUP)]
            for j in range(GROUP):
                left[h] = left[h] - rows[j] * g_left[j]
                right[h] = right[h] - rows[j] * g_right[j]
        left[g], right[g] = out_left, out_right
    return jnp.concatenate(left, 0), jnp.concatenate(right, 0)


def factor_kernel(width, a_ref, u_ref, m_ref):
    n = a_ref.shape[0]
    m_ref[:, :n] = a_ref[...]
    ids = lax.broadcasted_iota(jnp.int32, (n, n), 0) == lax.broadcasted_iota(jnp.int32, (n, n), 1)
    m_ref[:, n:] = jnp.where(ids, 1.0, 0.0)

    for k in range(n // width):
        at = k * width
        _, inverse = factor_block(m_ref[at : at + width, at : at + width])
        upper = jnp.dot(inverse, m_ref[at : at + width, :], precision=HIGH, preferred_element_type=jnp.float32)
        col_ids = lax.broadcasted_iota(jnp.int32, upper.shape, 1)
        row_ids = lax.broadcasted_iota(jnp.int32, upper.shape, 0) + at
        upper = jnp.where((col_ids >= row_ids) & (col_ids <= row_ids + n), upper, 0.0)
        u_ref[at : at + width, :] = upper
        if at + width < n:
            m_ref[at + width :, :] -= lax.dot_general(
                upper[:, at + width : n], upper, (((0,), (0,)), ((), ())),
                precision=HIGH, preferred_element_type=jnp.float32,
            )


def factor(a):
    n = a.shape[0]
    width = min(128, n)
    out = pl.pallas_call(
        functools.partial(factor_kernel, width),
        out_shape=jax.ShapeDtypeStruct((n, 2 * n), jnp.float32),
        in_specs=[pl.BlockSpec(memory_space=pltpu.VMEM)],
        out_specs=pl.BlockSpec(memory_space=pltpu.VMEM),
        scratch_shapes=[pltpu.VMEM((n, 2 * n), jnp.float32)],
        compiler_params=pltpu.CompilerParams(vmem_limit_bytes=48 * 1024 * 1024),
    )(a)
    return out[:, :n], out[:, n:]


def gram(a, b):
    return lax.dot_general(a, b, (((0,), (0,)), ((), ())), preferred_element_type=jnp.float32)


def spread(block, holder):
    return lax.psum(jnp.where(lax.axis_index("blk") == holder, block, 0), "blk")


def gather(activations, lead, strip_width):
    rows_block = activations.shape[1]
    tok_index = lax.axis_index("tok")
    own = lax.all_gather(activations, "tok", axis=0, tiled=True)
    start = tok_index * strip_width
    strip = lax.dynamic_slice_in_dim(own, lax.rem(start, rows_block), strip_width, 1)
    if lax.axis_size("blk") > 2:
        first = spread(own[:, :lead], 0)
        strip = spread(strip, start // rows_block)
    else:
        both = lax.all_gather(jnp.concatenate([own[:, :lead], strip], 1), "blk", axis=0)
        first = both[0, :, :lead]
        strip = lax.dynamic_index_in_dim(both, start // rows_block, 0, False)[:, lead:]
    square = jnp.sum(jnp.square(own.astype(jnp.float32)))
    squares = jnp.sum(lax.all_gather(jnp.broadcast_to(square, (8, 128)), "blk", axis=0)[:, 0, 0])
    return own, first, strip, squares


ORDERS = ("zyx", "zxy", "xzy", "yzx")
SIZES = {"z": 4, "y": 2, "x": 2}


def gather_kernel(lead, strip_width, act_ref, sq_in, own_ref, first_ref, strip_ref, sq_ref,
                  send, recv, push_send, push_recv, sq_send, sq_recv, local):
    tok = lax.axis_index("tok")
    blk = lax.axis_index("blk")
    count = lax.axis_size("tok")
    blks = lax.axis_size("blk")
    rows = act_ref.shape[0] // len(ORDERS)
    z, y, x = tok // 4, lax.rem(tok // 2, 2), lax.rem(tok, 2)
    me = tok * blks + blk
    total = count * blks

    barrier = pltpu.get_barrier_semaphore()

    def peer(i):
        other = lax.rem(me + i, total)
        return (other // blks, lax.rem(other, blks))

    def greet(i, carry):
        pl.semaphore_signal(barrier, inc=1, device_id=peer(i), device_id_type=pl.DeviceIdType.MESH)
        return carry

    lax.fori_loop(1, total, greet, 0)
    own_copy = pltpu.make_async_copy(act_ref, own_ref.at[tok], local.at[0])
    sq_copy = pltpu.make_async_copy(sq_in, sq_ref.at[me], local.at[1])
    own_copy.start()
    sq_copy.start()
    pl.semaphore_wait(barrier, total - 1)

    def index(dz, dy, dx):
        return (z + dz) * 4 + lax.rem(y + dy, 2) * 2 + lax.rem(x + dx, 2)

    def part(c):
        return pl.ds(c * rows, rows)

    def link(c, src, way, own):
        step = {"z+": (1, 0, 0), "z-": (-1, 0, 0), "y": (0, 1, 0), "x": (0, 0, 1)}[way]
        slot = ("z+", "z-", "y", "x").index(way)
        source = act_ref.at[part(c)] if own else own_ref.at[src, part(c)]
        return pltpu.make_async_remote_copy(
            src_ref=source,
            dst_ref=own_ref.at[src, part(c)],
            send_sem=send.at[c, slot, src],
            recv_sem=recv.at[c, src],
            device_id=(index(*step), blk),
            device_id_type=pl.DeviceIdType.MESH,
        )

    def ways(order, delta):
        last = -1
        for s, dim in enumerate(order):
            if delta["zyx".index(dim)]:
                last = s
        result = []
        for s, dim in enumerate(order):
            if s > last:
                result += ["z+", "z-"] if dim == "z" else [dim]
            elif s == last and dim == "z":
                result += ["z+"] if delta[0] < 0 else ["z-"]
        return result

    def guarded(way, body):
        if way == "z+":
            pl.when(z < 3)(body)
        elif way == "z-":
            pl.when(z > 0)(body)
        else:
            body()

    events = [(abs(dz) + dy + dx, c, (dz, dy, dx))
              for dz in range(-3, 4) for dy in range(2) for dx in range(2)
              for c in range(len(ORDERS))]
    events.sort(key=lambda e: (e[0], abs(e[2][0]), e[1]))

    def push(c, src, own):
        source = act_ref if own else own_ref.at[src]
        start = pl.multiple_of(lax.rem(tok * strip_width, act_ref.shape[1]), strip_width)
        for k, (take, goal) in enumerate(((pl.ds(0, lead), first_ref), (pl.ds(start, strip_width), strip_ref))):
            yield pltpu.make_async_remote_copy(
                src_ref=source.at[part(c), take],
                dst_ref=goal.at[src, part(c)],
                send_sem=push_send.at[k],
                recv_sem=push_recv.at[k],
                device_id=(tok, 1 - blk),
                device_id_type=pl.DeviceIdType.MESH,
            )

    def visit(event, wait):
        _, c, delta = event
        own = delta == (0, 0, 0)
        src = index(*delta)
        follow = ways(ORDERS[c], delta)

        def run():
            if wait:
                for way in follow:
                    guarded(way, lambda way=way: link(c, src, way, own).wait_send())
                return
            if not own:
                link(c, src, "x", False).wait_recv()
            for way in follow:
                guarded(way, lambda way=way: link(c, src, way, own).start())

            @pl.when(blk == 0)
            def _():
                for copy in push(c, src, own):
                    copy.start()

        if delta[0]:
            pl.when((z + delta[0] >= 0) & (z + delta[0] <= 3))(run)
        else:
            run()

    def sq_link(i):
        return pltpu.make_async_remote_copy(
            src_ref=sq_in,
            dst_ref=sq_ref.at[me],
            send_sem=sq_send.at[i],
            recv_sem=sq_recv,
            device_id=peer(i),
            device_id_type=pl.DeviceIdType.MESH,
        )

    for event in events[: len(ORDERS)]:
        visit(event, False)

    def sq_start(i, carry):
        sq_link(i).start()
        return carry

    lax.fori_loop(1, total, sq_start, 0)
    for event in events[len(ORDERS):]:
        visit(event, False)
    for event in events:
        visit(event, True)

    def sq_wait(i, carry):
        sq_link(i).wait_send()
        return carry

    lax.fori_loop(1, total, sq_wait, 0)
    rest = sq_ref.at[pl.ds(0, total - 1)]
    pltpu.make_async_copy(rest, rest, sq_recv).wait()
    own_copy.wait()
    sq_copy.wait()

    @pl.when(blk == 0)
    def _():
        for k, goal in enumerate((first_ref, strip_ref)):
            pltpu.make_async_copy(goal, goal, push_send.at[k]).wait()

    @pl.when(blk == 1)
    def _():
        for k, goal in enumerate((first_ref, strip_ref)):
            pltpu.make_async_copy(goal, goal, push_recv.at[k]).wait()


def gather_links(activations, lead, strip_width):
    rows, width = activations.shape
    count = lax.axis_size("tok")
    total = count * lax.axis_size("blk")
    tok_index = lax.axis_index("tok")
    blk_index = lax.axis_index("blk")
    square = jnp.sum(jnp.square(activations.astype(jnp.float32)))
    vmem = pl.BlockSpec(memory_space=pltpu.VMEM)
    dma = pltpu.SemaphoreType.DMA
    own, first, strip, squares = pl.pallas_call(
        functools.partial(gather_kernel, lead, strip_width),
        out_shape=[
            jax.ShapeDtypeStruct((count, rows, width), activations.dtype),
            jax.ShapeDtypeStruct((count, rows, lead), activations.dtype),
            jax.ShapeDtypeStruct((count, rows, strip_width), activations.dtype),
            jax.ShapeDtypeStruct((total, 8, 128), jnp.float32),
        ],
        in_specs=[vmem, vmem],
        out_specs=[vmem] * 4,
        scratch_shapes=[
            dma((len(ORDERS), 4, count)), dma((len(ORDERS), count)),
            dma((2,)), dma((2,)), dma((total,)), dma, dma((2,)),
        ],
        compiler_params=pltpu.CompilerParams(
            collective_id=0, has_side_effects=True, vmem_limit_bytes=40 * 1024 * 1024
        ),
    )(activations, jnp.broadcast_to(square, (8, 128)))
    own = own.reshape(count * rows, width)
    first = jnp.where(blk_index == 0, own[:, :lead], first.reshape(count * rows, lead))
    start = tok_index * strip_width
    mine = lax.dynamic_slice_in_dim(own, lax.rem(start, width), strip_width, 1)
    strip = jnp.where(blk_index == start // width, mine, strip.reshape(count * rows, strip_width))
    return own, first, strip, jnp.sum(squares[:, 0, 0])


def finish(own, first, strip, squares, sizes):
    rows_block, full_width, strip_width, lead, total_tokens = sizes
    tok_index = lax.axis_index("tok")
    blk_index = lax.axis_index("blk")
    scale = 2.0 / total_tokens
    damping = 0.01 * squares * scale / full_width
    corner = gram(first, first) * scale
    ids = jnp.arange(lead, dtype=jnp.int32)
    corner = corner + jnp.where(ids[:, None] == ids[None, :], damping, 0.0)
    upper, inverse = factor(corner)
    side = gram(own, first) * scale
    tile = gram(own, strip) * scale
    cross = gram(strip, first) * scale
    lower_rows = lax.dot_general(side, inverse, (((1,), (1,)), ((), ())), precision=HIGH)
    lower_cols = lax.dot_general(cross, inverse, (((1,), (1,)), ((), ())), precision=HIGH)
    row_ids = blk_index * rows_block + jnp.arange(rows_block, dtype=jnp.int32)[:, None]
    col_ids = tok_index * strip_width + jnp.arange(strip_width, dtype=jnp.int32)[None, :]
    schur = tile + jnp.where(row_ids == col_ids, damping, 0.0)
    schur = schur - lax.dot_general(lower_rows, lower_cols, (((1,), (1,)), ((), ())), precision=HIGH)
    at = jnp.minimum(tok_index * strip_width, lead - strip_width)
    leading = jnp.concatenate([upper.T, jnp.zeros((max(rows_block - lead, 0), lead), jnp.float32)], 0)
    head = jnp.where(row_ids < lead, leading, lower_rows)
    head = lax.dynamic_slice_in_dim(head, at, strip_width, 1)
    result = jnp.where(col_ids < lead, head, schur)
    return jnp.where((row_ids >= col_ids) & ((row_ids >= lead) | (col_ids < lead)), result, 0.0)


def shards(activations):
    rows_block = activations.shape[1]
    tok_count = lax.axis_size("tok")
    full_width = rows_block * lax.axis_size("blk")
    strip_width = full_width // tok_count
    lead = STEPS * strip_width
    total_tokens = activations.shape[0] * tok_count
    sizes = (rows_block, full_width, strip_width, lead, total_tokens)
    gathered = gather_links if (tok_count, lax.axis_size("blk")) == (16, 2) else gather
    return finish(*gathered(activations, lead, strip_width), sizes)


def solution(mesh):
    return jax.shard_map(
        shards,
        mesh=mesh,
        in_specs=(P("tok", "blk"),),
        out_specs=P("blk", "tok"),
        check_vma=False,
    )
```
